32 devices in a mesh: section: 4 (over z), dp: 2 (over x), mp: 4 (over y, core).
Axes of the slice: x: 2, y: 2, z: 4, core: 2. Of those that a mesh axis runs over, the one named last changes fastest.
Arguments:
- entrance: bfloat16 [2, 2, 96, 4096], P('dp'), may hold values from -6 to 6
- lengths: int32 [2, 2], P('dp'), may hold values from 24 to 96
- positives: int32 [2], replicated, may hold values from 0 to 1, each once
- norm_gains: float32 [4, 4096], P('section'), may hold values from 0.5 to 1.5
- query_proj: bfloat16 [4, 4096, 2048], P('section', None, 'mp'), may hold values from -0.09375 to 0.09375
- key_proj: bfloat16 [4, 4096, 512], P('section', None, 'mp'), may hold values from -0.09375 to 0.09375
- value_proj: bfloat16 [4, 4096, 512], P('section', None, 'mp'), may hold values from -0.09375 to 0.09375
- out_proj: bfloat16 [4, 2048, 4096], P('section', 'mp'), may hold values from -0.125 to 0.125
Outputs:
- losses: float32 [4, 7], P('section')
- norm_gain_grad: float32 [4, 4096], P('section', ('dp', 'mp'))
- query_proj_grad: float32 [4, 4096, 2048], P('section', 'dp', 'mp')
- key_proj_grad: float32 [4, 4096, 512], P('section', 'dp', 'mp')
- value_proj_grad: float32 [4, 4096, 512], P('section', 'dp', 'mp')
- out_proj_grad: float32 [4, 2048, 4096], P('section', 'mp', 'dp')
The draws below stay inside these ranges and needn't reach their ends.
Inputs may be any that keep to these rules, and one draw needn't show every extreme that they name: positives is a permutation of the pair indices. `lengths`: tokens at or past a sequence's length are padding.
All inputs are finite; a program needn't handle non-finite values.
Results may differ from the reference program's by a relative error of at most 0.039.
Values may be sent and summed in bfloat16 or wider, within the bound.
A program may use at most 128 MiB of HBM per device.

```python
import jax
import jax.numpy as jnp
from jax import lax

D = 4096
HQ = 16
HK = 4
HEAD = 128
WIDTHS = 7
LEN = 96
PAIRS = 2
N_SECTION = 4
N_MP = 4


def with_ends(entries, stream_key, low, high):
    longest = entries.shape.index(max(entries.shape))
    spots = []
    for shift in (0, 1):
        where = [jax.random.randint(jax.random.fold_in(stream_key, axis), (), 0, length) for axis, length in enumerate(entries.shape)]
        where[longest] = (where[longest] + shift) % entries.shape[longest]
        spots.append(tuple(where))
    return entries.at[spots[0]].set(low).at[spots[1]].set(high)


def block_levels(rng, shape, split, low, largest):
    loudness = 1.0
    for axis_at, shards_of in split:
        heights = jax.random.uniform(jax.random.fold_in(jax.random.fold_in(rng, 6), axis_at), (shards_of,), jnp.float32, low / len(split), largest / len(split))
        loudness = loudness * jnp.repeat(jnp.exp(heights), shape[axis_at] // shards_of).reshape((-1,) + (1,) * (len(shape) - 1 - axis_at))
    return loudness


def gaussian(stream_key, dims, spread, limit, split=(), held_as=jnp.bfloat16):
    loudness = block_levels(stream_key, dims, split, -0.22, 0.18) if split else 1.0
    values = jax.random.normal(stream_key, dims, jnp.float32) * spread * loudness
    return jnp.minimum(jnp.maximum(values, -limit), limit).astype(held_as)


def setup_inputs(seed: int = 0) -> dict:
    seeds = jax.random.split(jax.random.key(seed), 9)
    entrance = gaussian(seeds[0], (PAIRS, 2, LEN, D), 1.0, 6.0, ((0, 2),))
    lengths = with_ends(jax.random.randint(seeds[1], (PAIRS, 2), LEN // 4, LEN + 1), jax.random.fold_in(seeds[1], 1), LEN // 4, LEN).astype(jnp.int32)
    positives = jax.random.permutation(seeds[2], PAIRS).astype(jnp.int32)
    norm_gains = jnp.clip(1.0 + 0.1 * jax.random.normal(seeds[3], (N_SECTION, D), jnp.float32), 0.5, 1.5)
    query_proj = gaussian(seeds[4], (N_SECTION, D, HQ * HEAD), D ** -0.5, 0.09375, ((0, 4), (2, 4)))
    key_proj = gaussian(seeds[5], (N_SECTION, D, HK * HEAD), D ** -0.5, 0.09375, ((0, 4), (2, 4)))
    value_proj = gaussian(seeds[6], (N_SECTION, D, HK * HEAD), D ** -0.5, 0.09375, ((0, 4), (2, 4)))
    out_proj = gaussian(seeds[7], (N_SECTION, HQ * HEAD, D), (HQ * HEAD) ** -0.5, 0.125, ((0, 4), (1, 4)))
    return dict(entrance=entrance, lengths=lengths, positives=positives, norm_gains=norm_gains, query_proj=query_proj, key_proj=key_proj, value_proj=value_proj, out_proj=out_proj)


EPSILON = 1e-05
SOFTMAX_TEMPER = 0.05
ROPE_BASE = 500000.0

def rope_tables(length, head_size):
    half_size = head_size // 2
    inverse_freq = ROPE_BASE ** (-jnp.arange(half_size, dtype=jnp.float32) * 2.0 / head_size)
    angles = jnp.arange(length, dtype=jnp.float32)[:, None] * inverse_freq[None, :]
    return (jnp.cos(angles), jnp.sin(angles))

def rotate(values, cosine, sine_table):
    half_size = values.shape[-1] // 2
    first_half = values[..., :half_size]
    second = values[..., half_size:]
    cosine = cosine[None, :, None, :]
    sine_table = sine_table[None, :, None, :]
    return jnp.concatenate([first_half * cosine - second * sine_table, second * cosine + first_half * sine_table], axis=-1)

def attend(query_pre, key_pre, value_pre):
    seq_count, length, query_width = query_pre.shape
    query_heads = query_width // HEAD
    kv_heads = key_pre.shape[-1] // HEAD
    group_size = query_heads // kv_heads
    cosine, sine_table = rope_tables(length, HEAD)
    query_vectors = rotate(query_pre.reshape(seq_count, length, query_heads, HEAD), cosine, sine_table).astype(jnp.bfloat16)
    key_rows = rotate(key_pre.reshape(seq_count, length, kv_heads, HEAD), cosine, sine_table).astype(jnp.bfloat16)
    values = value_pre.reshape(seq_count, length, kv_heads, HEAD).astype(jnp.bfloat16)
    query_vectors = query_vectors.reshape(seq_count, length, kv_heads, group_size, HEAD)
    scores = jnp.einsum('sikge,sjke->skgij', query_vectors.astype(jnp.float32), key_rows.astype(jnp.float32)) * HEAD ** (-0.5)
    causal = jnp.arange(length, dtype=jnp.int32)[:, None] >= jnp.arange(length, dtype=jnp.int32)[None, :]
    scores = jnp.where(causal, scores, -1e+30)
    weights = jax.nn.softmax(scores, axis=-1).astype(jnp.bfloat16)
    mixture = jnp.einsum('skgij,sjke->sikge', weights.astype(jnp.float32), values.astype(jnp.float32))
    return mixture.reshape(seq_count, length, query_heads * HEAD)

def normalize(hidden_f, gain_vector):
    inv_rms = lax.rsqrt(lax.optimization_barrier(jnp.mean(hidden_f * hidden_f, axis=-1, keepdims=True)) + EPSILON)
    return hidden_f * inv_rms * gain_vector

def contract_rows(left, right):
    return lax.dot_general(left, right, (((0,), (0,)), ((), ())), preferred_element_type=jnp.float32)

def contract_last(left, right):
    return lax.dot_general(left, right, (((left.ndim - 1,), (1,)), ((), ())), preferred_element_type=jnp.float32)

def pool_exits(batch_rows, mask_of_valid, counts):
    total_value = jnp.einsum('ki,kiu->ku', mask_of_valid, batch_rows.astype(jnp.float32))
    return total_value / counts[:, None]

def spread_grad(exit_grad, mask_of_valid, counts):
    return mask_of_valid[:, :, None] * (exit_grad / counts[:, None])[:, None, :]

def matryoshka_losses(pooled, positives):
    pair_total = pooled.shape[0]
    target = (jnp.arange(pair_total, dtype=jnp.int32)[None, :] == positives[:, None]).astype(jnp.float32)
    losses = []
    for level_index in range(WIDTHS):
        leading_width = pooled.shape[-1] // 2 ** level_index
        query_vectors = pooled[:, 0, :leading_width]
        passage_rows = pooled[:, 1, :leading_width]
        query_vectors = query_vectors * lax.rsqrt(lax.optimization_barrier(jnp.mean(query_vectors * query_vectors, axis=-1, keepdims=True)) + 1e-06)
        passage_rows = passage_rows * lax.rsqrt(lax.optimization_barrier(jnp.mean(passage_rows * passage_rows, axis=-1, keepdims=True)) + 1e-06)
        score_matrix = jnp.dot(query_vectors, passage_rows.T, precision=lax.Precision.HIGHEST) / (leading_width * SOFTMAX_TEMPER)
        picked = lax.optimization_barrier(jnp.sum(score_matrix * target, axis=-1))
        losses.append(jnp.mean(jax.nn.logsumexp(score_matrix, axis=-1) - picked))
    return jnp.stack(losses)

def section_forward(hidden, gain_vector, query_weight, key_weight, value_weight, out_weight):
    hidden_f = hidden.astype(jnp.float32)
    normed = normalize(hidden_f, gain_vector).astype(jnp.bfloat16)
    query_cols = query_weight.shape[1] // N_MP
    kv_cols = key_weight.shape[1] // N_MP
    total_value = jnp.zeros(hidden_f.shape, jnp.float32)
    for member in range(N_MP):
        query_slice = query_weight[:, member * query_cols:(member + 1) * query_cols]
        key_slice = key_weight[:, member * kv_cols:(member + 1) * kv_cols]
        value_slice = value_weight[:, member * kv_cols:(member + 1) * kv_cols]
        out_slice = out_weight[member * query_cols:(member + 1) * query_cols]
        mixture = attend(jnp.dot(normed, query_slice, preferred_element_type=jnp.float32), jnp.dot(normed, key_slice, preferred_element_type=jnp.float32), jnp.dot(normed, value_slice, preferred_element_type=jnp.float32)).astype(jnp.bfloat16)
        partial_value = jnp.dot(mixture, out_slice, preferred_element_type=jnp.float32).astype(jnp.bfloat16)
        total_value = total_value + partial_value.astype(jnp.float32)
    return (hidden_f + total_value).astype(jnp.bfloat16)

def section_backward(hidden, upstream, gain_vector, query_weight, key_weight, value_weight, out_weight):
    hidden_f = hidden.astype(jnp.float32)
    inv_rms = lax.rsqrt(lax.optimization_barrier(jnp.mean(hidden_f * hidden_f, axis=-1, keepdims=True)) + EPSILON)
    normed = normalize(hidden_f, gain_vector).astype(jnp.bfloat16)
    out_grad = upstream.astype(jnp.bfloat16)
    query_cols = query_weight.shape[1] // N_MP
    kv_cols = key_weight.shape[1] // N_MP
    width_all = hidden.shape[-1]
    normed_rows = normed.reshape(-1, width_all)
    out_rows = out_grad.reshape(-1, width_all)
    normed_grad = jnp.zeros(hidden_f.shape, jnp.float32)
    query_parts, key_parts, value_parts, out_parts = ([], [], [], [])
    for member in range(N_MP):
        query_slice = query_weight[:, member * query_cols:(member + 1) * query_cols]
        key_slice = key_weight[:, member * kv_cols:(member + 1) * kv_cols]
        value_slice = value_weight[:, member * kv_cols:(member + 1) * kv_cols]
        out_slice = out_weight[member * query_cols:(member + 1) * query_cols]
        mixture_f, pullback = jax.vjp(attend, jnp.dot(normed, query_slice, preferred_element_type=jnp.float32), jnp.dot(normed, key_slice, preferred_element_type=jnp.float32), jnp.dot(normed, value_slice, preferred_element_type=jnp.float32))
        mixture = mixture_f.astype(jnp.bfloat16)
        mixture_grad = contract_last(out_grad, out_slice).astype(jnp.bfloat16)
        pulled = pullback(lax.optimization_barrier(mixture_grad).astype(jnp.float32))
        query_grad, key_grad, value_grad = [piece_grad.astype(jnp.bfloat16) for piece_grad in pulled]
        member_grad = contract_last(query_grad, query_slice) + contract_last(key_grad, key_slice) + contract_last(value_grad, value_slice)
        normed_grad = normed_grad + lax.optimization_barrier(member_grad.astype(jnp.bfloat16)).astype(jnp.float32)
        query_parts.append(contract_rows(normed_rows, query_grad.reshape(-1, query_cols)))
        key_parts.append(contract_rows(normed_rows, key_grad.reshape(-1, kv_cols)))
        value_parts.append(contract_rows(normed_rows, value_grad.reshape(-1, kv_cols)))
        out_parts.append(contract_rows(mixture.reshape(-1, query_cols), out_rows))
    gain_grad = lax.optimization_barrier(jnp.sum(normed_grad * hidden_f * inv_rms, axis=(0, 1)))
    _, norm_pull = jax.vjp(lambda values: normalize(values, gain_vector), hidden_f)
    input_grad = (upstream + norm_pull(normed_grad)[0]).astype(jnp.bfloat16)
    return (input_grad, (gain_grad, jnp.concatenate(query_parts, axis=1), jnp.concatenate(key_parts, axis=1), jnp.concatenate(value_parts, axis=1), jnp.concatenate(out_parts, axis=0)))

def reference(entrance, lengths, positives, norm_gains, query_proj, key_proj, value_proj, out_proj):
    seq_count = 2 * PAIRS
    hidden = entrance.reshape(seq_count, LEN, D)
    mask_of_valid = (jnp.arange(LEN, dtype=jnp.int32)[None, :] < lengths.reshape(seq_count, 1)).astype(jnp.float32)
    counts = lax.optimization_barrier(jnp.sum(mask_of_valid, axis=1))
    section_inputs = []
    loss_rows = []
    token_grads = []
    for section_index in range(N_SECTION):
        section_inputs.append(hidden)
        hidden = section_forward(hidden, norm_gains[section_index], query_proj[section_index], key_proj[section_index], value_proj[section_index], out_proj[section_index])
        pooled = pool_exits(hidden, mask_of_valid, counts).reshape(PAIRS, 2, D)
        losses_now, pullback = jax.vjp(lambda embedded: matryoshka_losses(embedded, positives), pooled)
        exit_grad = pullback(jnp.ones((WIDTHS,), jnp.float32))[0]
        loss_rows.append(losses_now)
        token_grads.append(spread_grad(exit_grad.reshape(seq_count, D), mask_of_valid, counts))
    incoming = jnp.zeros((seq_count, LEN, D), jnp.bfloat16)
    results = [None] * N_SECTION
    for section_index in reversed(range(N_SECTION)):
        upstream = token_grads[section_index] + incoming.astype(jnp.float32)
        incoming, grads_now = section_backward(section_inputs[section_index], upstream, norm_gains[section_index], query_proj[section_index], key_proj[section_index], value_proj[section_index], out_proj[section_index])
        results[section_index] = grads_now
    return (jnp.stack(loss_rows), jnp.stack([entry[0] for entry in results]), jnp.stack([entry[1] for entry in results]), jnp.stack([entry[2] for entry in results]), jnp.stack([entry[3] for entry in results]), jnp.stack([entry[4] for entry in results]))
```

```python
import functools

import jax
import jax.numpy as jnp
from jax import lax
from jax.experimental import pallas as pl
from jax.experimental.pallas import tpu as pltpu
from jax.sharding import PartitionSpec as P

HEAD = 128
WIDTHS = 7


EPSILON = 1e-05
SOFTMAX_TEMPER = 0.05
ROPE_BASE = 500000.0


def rope_tables(length, head_size):
    half_size = head_size // 2
    inverse_freq = ROPE_BASE ** (-jnp.arange(half_size, dtype=jnp.float32) * 2.0 / head_size)
    angles = jnp.arange(length, dtype=jnp.float32)[:, None] * inverse_freq[None, :]
    return (jnp.cos(angles), jnp.sin(angles))


def rotate(values, cosine, sine_table):
    half_size = values.shape[-1] // 2
    first_half = values[..., :half_size]
    second = values[..., half_size:]
    cosine = cosine[None, :, None, :]
    sine_table = sine_table[None, :, None, :]
    return jnp.concatenate(
        [first_half * cosine - second * sine_table, second * cosine + first_half * sine_table],
        axis=-1,
    )


def attend(query_pre, key_pre, value_pre):
    seq_count, length, query_width = query_pre.shape
    query_heads = query_width // HEAD
    kv_heads = key_pre.shape[-1] // HEAD
    group_size = query_heads // kv_heads
    cosine, sine_table = rope_tables(length, HEAD)
    query_vectors = rotate(
        query_pre.reshape(seq_count, length, query_heads, HEAD), cosine, sine_table
    ).astype(jnp.bfloat16)
    key_rows = rotate(
        key_pre.reshape(seq_count, length, kv_heads, HEAD), cosine, sine_table
    ).astype(jnp.bfloat16)
    values = value_pre.reshape(seq_count, length, kv_heads, HEAD).astype(jnp.bfloat16)
    query_vectors = query_vectors.reshape(seq_count, length, kv_heads, group_size, HEAD)
    scores = jnp.einsum(
        "sikge,sjke->skgij", query_vectors.astype(jnp.float32), key_rows.astype(jnp.float32)
    ) * HEAD ** (-0.5)
    causal = (
        jnp.arange(length, dtype=jnp.int32)[:, None] >= jnp.arange(length, dtype=jnp.int32)[None, :]
    )
    scores = jnp.where(causal, scores, -1e30)
    weights = jax.nn.softmax(scores, axis=-1).astype(jnp.bfloat16)
    mixture = jnp.einsum(
        "skgij,sjke->sikge", weights.astype(jnp.float32), values.astype(jnp.float32)
    )
    return mixture.reshape(seq_count, length, query_heads * HEAD)


def normalize(hidden_f, gain_vector):
    inv_rms = lax.rsqrt(jnp.mean(hidden_f * hidden_f, axis=-1, keepdims=True) + EPSILON)
    return hidden_f * inv_rms * gain_vector


def contract_rows(left, right):
    return lax.dot_general(
        left, right, (((0,), (0,)), ((), ())), preferred_element_type=jnp.float32
    )


def contract_last(left, right):
    return lax.dot_general(
        left, right, (((left.ndim - 1,), (1,)), ((), ())), preferred_element_type=jnp.float32
    )


def spread_grad(exit_grad, mask_of_valid, counts):
    return mask_of_valid[:, :, None] * (exit_grad / counts[:, None])[:, None, :]


def matryoshka_losses(pooled, positives):
    pair_total = pooled.shape[0]
    target = (jnp.arange(pair_total, dtype=jnp.int32)[None, :] == positives[:, None]).astype(
        jnp.float32
    )
    losses = []
    for level_index in range(WIDTHS):
        leading_width = pooled.shape[-1] // 2**level_index
        query_vectors = pooled[:, 0, :leading_width]
        passage_rows = pooled[:, 1, :leading_width]
        query_vectors = query_vectors * lax.rsqrt(
            jnp.mean(query_vectors * query_vectors, axis=-1, keepdims=True) + 1e-06
        )
        passage_rows = passage_rows * lax.rsqrt(
            jnp.mean(passage_rows * passage_rows, axis=-1, keepdims=True) + 1e-06
        )
        score_matrix = jnp.dot(query_vectors, passage_rows.T, precision=lax.Precision.HIGHEST) / (
            leading_width * SOFTMAX_TEMPER
        )
        picked = jnp.sum(score_matrix * target, axis=-1)
        losses.append(jnp.mean(jax.nn.logsumexp(score_matrix, axis=-1) - picked))
    return jnp.stack(losses)


MESH = pl.DeviceIdType.MESH
ROW_TILE = 16


def mp_place(me, levels):
    bits = [(me // (1 << level)) % 2 for level in range(levels)]
    partners = [me + (1 - 2 * bits[level]) * (1 << level) for level in range(levels)]
    return bits, partners


def shard_offset(bits, rows, flips=0):
    offset = 0
    for level, bit in enumerate(bits):
        bit = 1 - bit if (flips >> level) & 1 else bit
        offset = offset + bit * (rows >> (level + 1))
    return offset


def rows_at(start, size):
    return pl.ds(pl.multiple_of(start, ROW_TILE), size)


def scatter_kernel(levels, part_ref, out_ref, *scratch):
    arrived, kept = scratch[:levels], scratch[levels : 2 * levels - 1]
    send_sem, recv_sem = scratch[2 * levels - 1 :]
    bits, partners = mp_place(lax.axis_index("mp"), levels)
    barrier = pltpu.get_barrier_semaphore()
    for partner in partners:
        pl.semaphore_signal(barrier, inc=1, device_id={"mp": partner}, device_id_type=MESH)
    pl.semaphore_wait(barrier, levels)
    held = part_ref
    for level in range(levels):
        half = held.shape[0] // 2
        copy = pltpu.make_async_remote_copy(
            src_ref=held.at[rows_at((1 - bits[level]) * half, half)],
            dst_ref=arrived[level],
            send_sem=send_sem.at[level],
            recv_sem=recv_sem.at[level],
            device_id={"mp": partners[level]},
            device_id_type=MESH,
        )
        copy.start()
        copy.wait()
        target = out_ref if level == levels - 1 else kept[level]

        def add(step, carry, held=held, half=half, target=target, level=level):
            own = held[rows_at(bits[level] * half + step * ROW_TILE, ROW_TILE), :]
            other = arrived[level][rows_at(step * ROW_TILE, ROW_TILE), :]
            total = own.astype(jnp.float32) + other.astype(jnp.float32)
            target[rows_at(step * ROW_TILE, ROW_TILE), :] = total.astype(target.dtype)
            return carry

        lax.fori_loop(0, half // ROW_TILE, add, 0)
        held = target


def scatter_rows(partial_value):
    rows, width = partial_value.shape
    members = lax.axis_size("mp")
    levels = members.bit_length() - 1
    arrived = [pltpu.VMEM((rows >> (level + 1), width), jnp.bfloat16) for level in range(levels)]
    return pl.pallas_call(
        functools.partial(scatter_kernel, levels),
        out_shape=jax.ShapeDtypeStruct((rows // members, width), jnp.float32),
        in_specs=[pl.BlockSpec(memory_space=pltpu.VMEM)],
        out_specs=pl.BlockSpec(memory_space=pltpu.VMEM),
        scratch_shapes=arrived
        + arrived[:-1]
        + [pltpu.SemaphoreType.DMA((levels,)), pltpu.SemaphoreType.DMA((levels,))],
        compiler_params=pltpu.CompilerParams(collective_id=0, has_side_effects=True),
        name="scatter_rows",
    )(partial_value)


def relay_kernel(levels, direction, shard_ref, out_ref, relay_send, relay_recv, send_sem, recv_sem):
    members = 1 << levels
    shard_rows = shard_ref.shape[0]
    rows = out_ref.shape[0]
    chunks = shard_rows // ROW_TILE
    here = lax.axis_index("section")
    count = lax.axis_size("section")
    if direction > 0:
        has_source, has_target = here > 0, here < count - 1
    else:
        has_source, has_target = here < count - 1, here > 0
    bits, partners = mp_place(lax.axis_index("mp"), levels)
    barrier = pltpu.get_barrier_semaphore()

    @pl.when(has_source)
    def _():
        pl.semaphore_signal(
            barrier, inc=1, device_id={"section": here - direction}, device_id_type=MESH
        )
        for partner in partners:
            pl.semaphore_signal(barrier, inc=1, device_id={"mp": partner}, device_id_type=MESH)

    @pl.when(jnp.logical_and(has_source, has_target))
    def _():
        pl.semaphore_wait(barrier, levels + 1)

    @pl.when(jnp.logical_and(has_source, jnp.logical_not(has_target)))
    def _():
        pl.semaphore_wait(barrier, levels)

    @pl.when(jnp.logical_and(has_target, jnp.logical_not(has_source)))
    def _():
        pl.semaphore_wait(barrier, 1)

    def piece(chunk, flips):
        return out_ref.at[rows_at(shard_offset(bits, rows, flips) + chunk * ROW_TILE, ROW_TILE)]

    def relay(chunk):
        return pltpu.make_async_remote_copy(
            src_ref=shard_ref.at[pl.ds(chunk * ROW_TILE, ROW_TILE)],
            dst_ref=piece(chunk, 0),
            send_sem=relay_send.at[chunk],
            recv_sem=relay_recv.at[chunk],
            device_id={"section": here + direction},
            device_id_type=MESH,
        )

    def spread(chunk, flips, level):
        slot = (flips | (1 << level)) - 1
        return pltpu.make_async_remote_copy(
            src_ref=piece(chunk, flips),
            dst_ref=piece(chunk, flips),
            send_sem=send_sem.at[chunk, slot],
            recv_sem=recv_sem.at[chunk, slot],
            device_id={"mp": partners[level]},
            device_id_type=MESH,
        )

    def incoming(chunk, flips):
        level = (flips & -flips).bit_length() - 1
        return pltpu.make_async_remote_copy(
            src_ref=piece(chunk, flips),
            dst_ref=piece(chunk, flips),
            send_sem=send_sem.at[chunk, flips - 1],
            recv_sem=recv_sem.at[chunk, flips - 1],
            device_id={"mp": partners[level]},
            device_id_type=MESH,
        )

    @pl.when(has_target)
    def _():
        for chunk in range(chunks):
            relay(chunk).start()

    @pl.when(has_source)
    def _():
        sent = []
        order = sorted(range(1, members), key=lambda flips: -(flips & -flips))
        for chunk in range(chunks):
            relay(chunk).wait_recv()
            for level in reversed(range(levels)):
                copy = spread(chunk, 0, level)
                copy.start()
                sent.append(copy)
        for chunk in range(chunks):
            for flips in order:
                incoming(chunk, flips).wait_recv()
                lowest = (flips & -flips).bit_length() - 1
                for level in reversed(range(lowest)):
                    copy = spread(chunk, flips, level)
                    copy.start()
                    sent.append(copy)
        for copy in sent:
            copy.wait_send()

    @pl.when(jnp.logical_not(has_source))
    def _():
        def clear(step, carry):
            out_ref[rows_at(step * ROW_TILE, ROW_TILE), :] = jnp.zeros(
                (ROW_TILE, out_ref.shape[1]), out_ref.dtype
            )
            return carry

        lax.fori_loop(0, rows // ROW_TILE, clear, 0)

    @pl.when(has_target)
    def _():
        for chunk in range(chunks):
            relay(chunk).wait_send()


def relay_rows(shard, direction):
    shard_rows, width = shard.shape
    members = lax.axis_size("mp")
    levels = members.bit_length() - 1
    chunks = shard_rows // ROW_TILE
    return pl.pallas_call(
        functools.partial(relay_kernel, levels, direction),
        out_shape=jax.ShapeDtypeStruct((shard_rows * members, width), jnp.bfloat16),
        in_specs=[pl.BlockSpec(memory_space=pltpu.VMEM)],
        out_specs=pl.BlockSpec(memory_space=pltpu.VMEM),
        scratch_shapes=[
            pltpu.SemaphoreType.DMA((chunks,)),
            pltpu.SemaphoreType.DMA((chunks,)),
            pltpu.SemaphoreType.DMA((chunks, members - 1)),
            pltpu.SemaphoreType.DMA((chunks, members - 1)),
        ],
        compiler_params=pltpu.CompilerParams(
            collective_id=1 if direction > 0 else 2, has_side_effects=True
        ),
        name="relay_forward" if direction > 0 else "relay_backward",
    )(shard)


def local(entrance, lengths, positives, norm_gains, query_proj, key_proj, value_proj, out_proj):
    section_count = lax.axis_size("section")
    section_index = lax.axis_index("section")
    member_count = lax.axis_size("mp")
    dp_count = lax.axis_size("dp")
    pair_count = entrance.shape[0]
    seq_count = 2 * pair_count
    length = entrance.shape[2]
    width_all = entrance.shape[3]
    rows = seq_count * length
    shard_rows = rows // member_count
    bits, _ = mp_place(lax.axis_index("mp"), member_count.bit_length() - 1)
    offset = shard_offset(bits, rows)
    start_hidden = entrance.reshape(rows, width_all)
    mask_of_valid = (
        jnp.arange(length, dtype=jnp.int32)[None, :] < lengths.reshape(seq_count, 1)
    ).astype(jnp.float32)
    counts = jnp.sum(mask_of_valid, axis=1)
    gain_vector = norm_gains[0]
    head_weight = jnp.concatenate([query_proj[0], key_proj[0], value_proj[0]], axis=1)
    out_weight = out_proj[0]
    query_cols = query_proj.shape[2]
    kv_cols = key_proj.shape[2]

    def own_rows(values):
        return lax.dynamic_slice_in_dim(values, offset, shard_rows, 0)

    def attend_heads(heads):
        heads = heads.reshape(seq_count, length, -1)
        mixed = attend(
            heads[..., :query_cols],
            heads[..., query_cols : query_cols + kv_cols],
            heads[..., query_cols + kv_cols :],
        )
        return mixed.reshape(rows, -1)

    current = start_hidden
    for section_turn in range(section_count):
        normed = normalize(current.astype(jnp.float32), gain_vector).astype(jnp.bfloat16)
        heads = jnp.dot(normed, head_weight, preferred_element_type=jnp.float32)
        if section_turn + 1 == section_count:
            break
        mixture = attend_heads(heads).astype(jnp.bfloat16)
        partial_value = jnp.dot(mixture, out_weight, preferred_element_type=jnp.float32)
        total_value = scatter_rows(partial_value.astype(jnp.bfloat16))
        produced = own_rows(current).astype(jnp.float32) + total_value
        arrived = relay_rows(produced.astype(jnp.bfloat16), 1)
        current = jnp.where(section_index == 0, start_hidden, arrived)
    mixture_f, attend_pull = jax.vjp(attend_heads, heads)
    mixture = mixture_f.astype(jnp.bfloat16)
    hidden_f = current.astype(jnp.float32)
    inv_rms = lax.rsqrt(jnp.mean(hidden_f * hidden_f, axis=-1, keepdims=True) + EPSILON)

    token_mask = mask_of_valid[:, :, None]
    mixture_sum = jnp.sum(
        mixture.astype(jnp.float32).reshape(seq_count, length, -1) * token_mask, axis=1
    )
    coarse = mixture_sum.astype(jnp.bfloat16)
    fine = (mixture_sum - coarse.astype(jnp.float32)).astype(jnp.bfloat16)
    both = jnp.dot(
        jnp.concatenate([coarse, fine], axis=0), out_weight, preferred_element_type=jnp.float32
    )
    hidden_sum = jnp.sum(hidden_f.reshape(seq_count, length, -1) * token_mask, axis=1)
    pooled = both[:seq_count] + both[seq_count:]
    pooled = pooled + jnp.where(lax.axis_index("mp") == 0, hidden_sum, 0.0)
    pooled = pooled / counts[:, None]
    gathered = lax.all_gather(pooled, ("dp", "mp"), axis=0)
    gathered = jnp.sum(gathered.reshape(dp_count, member_count, seq_count, width_all), axis=1)
    gathered = gathered.reshape(dp_count * pair_count, 2, width_all)
    losses_now, pullback = jax.vjp(
        lambda embedded: matryoshka_losses(embedded, positives), gathered
    )
    pair_grads = pullback(jnp.ones((WIDTHS,), jnp.float32))[0]
    own_grad = lax.dynamic_slice_in_dim(
        pair_grads, lax.axis_index("dp") * pair_count, pair_count, 0
    )
    token_grad = spread_grad(own_grad.reshape(seq_count, width_all), mask_of_valid, counts)
    token_grad = token_grad.reshape(rows, width_all)

    normed_cols = lax.all_to_all(normed, "dp", split_axis=1, concat_axis=0, tiled=True)
    mixture_piece = lax.all_gather(mixture, "dp", axis=0, tiled=True)
    shard_hidden = own_rows(current).astype(jnp.float32)
    _, norm_pull = jax.vjp(lambda values: normalize(values, gain_vector), shard_hidden)
    upstream = token_grad
    for section_turn in range(section_count):
        out_grad = upstream.astype(jnp.bfloat16)
        mixture_grad = contract_last(out_grad, out_weight).astype(jnp.bfloat16)
        pulled = attend_pull(lax.optimization_barrier(mixture_grad).astype(jnp.float32))[0]
        head_grads = pulled.astype(jnp.bfloat16)
        member_grad = contract_last(head_grads, head_weight).astype(jnp.bfloat16)
        if section_turn + 1 == section_count:
            break
        normed_grad = scatter_rows(member_grad)
        input_grad = (own_rows(upstream) + norm_pull(normed_grad)[0]).astype(jnp.bfloat16)
        arrived = relay_rows(input_grad, -1).astype(jnp.float32)
        upstream = token_grad + jnp.where(section_index == section_count - 1, 0.0, arrived)
    out_cols = lax.all_to_all(out_grad, "dp", split_axis=1, concat_axis=0, tiled=True)
    head_piece = lax.all_gather(head_grads, "dp", axis=0, tiled=True)
    gain_term = jnp.sum(member_grad.astype(jnp.float32) * hidden_f * inv_rms, axis=0)
    gain_parts = lax.all_to_all(
        gain_term.reshape(dp_count * member_count, -1),
        ("dp", "mp"),
        split_axis=0,
        concat_axis=0,
        tiled=True,
    )
    gain_share = jnp.sum(gain_parts, axis=0)
    return (
        losses_now[None],
        gain_share[None],
        contract_rows(normed_cols, head_piece[:, :query_cols])[None],
        contract_rows(normed_cols, head_piece[:, query_cols : query_cols + kv_cols])[None],
        contract_rows(normed_cols, head_piece[:, query_cols + kv_cols :])[None],
        contract_rows(mixture_piece, out_cols)[None],
    )


def solution(mesh):
    in_specs = (
        P("dp", None, None, None),
        P("dp", None),
        P(),
        P("section", None),
        P("section", None, "mp"),
        P("section", None, "mp"),
        P("section", None, "mp"),
        P("section", "mp", None),
    )
    out_specs = (
        P("section", None),
        P("section", ("dp", "mp")),
        P("section", "dp", "mp"),
        P("section", "dp", "mp"),
        P("section", "dp", "mp"),
        P("section", "mp", "dp"),
    )
    return jax.shard_map(local, mesh=mesh, in_specs=in_specs, out_specs=out_specs, check_vma=False)
```
